128 devices in a mesh: rows: 128 (over z, y, x, core).
Axes of the slice: x: 4, y: 4, z: 4, core: 2. Of those that a mesh axis runs over, the one named last changes fastest.
Arguments:
- events: float32 [4, 32, 1048576], P(None, None, 'rows'), may hold values from -8 to 8
- keep_indicator: int32 [4, 1048576], P(None, 'rows'), may hold values from 0 to 1, as said below
Outputs:
- lagging_mean: float32 [4, 32, 1048576], P(None, None, 'rows')
- deviation: float32 [4, 32, 1048576], P(None, None, 'rows')
The draws below stay inside these ranges and needn't reach their ends.
Inputs may be any that keep to these rules, and one draw needn't show every extreme that they name: `keep_indicator`: in each table, each of the 128 aligned blocks of 8192 rows holds at least 4096 survivors, and some block holds exactly 4096.
All inputs are finite; a program needn't handle non-finite values.
Results may differ from the reference program's by a relative error of at most 0.0003.
Values sent between devices are 32-bit elements; how exact they have to be, the bound alone decides.
A program may use at most 128 MiB of HBM per device.

```python
import jax
import jax.numpy as jnp
from jax import lax

COLS = 32
SPAN_LENGTH = 4096
STREAMS = 4
ROWS_DEV = 8192
N_ROWS = 128


def draw_events(key, part):
    noise_key, level_key = jax.random.split(jax.random.fold_in(key, 11), 2)
    shape = (STREAMS, COLS, ROWS_DEV * N_ROWS)
    noise = jax.random.truncated_normal(noise_key, -4.0, 4.0, shape, jnp.float32)
    levels = jax.random.uniform(level_key, (STREAMS, 1, N_ROWS), jnp.float32, -2.0, 2.0)
    levels = jnp.broadcast_to(levels, (STREAMS, COLS, N_ROWS))
    spread = jnp.repeat(levels, ROWS_DEV, axis=2, total_repeat_length=ROWS_DEV * N_ROWS)
    return (noise + spread).astype(jnp.float32)


def draw_keep_indicator(key, part):
    count_key, perm_key, forced_key = jax.random.split(jax.random.fold_in(key, 23), 3)
    draws = jax.random.randint(count_key, (STREAMS, N_ROWS, 2), 0, ROWS_DEV - SPAN_LENGTH + 1)
    keep = SPAN_LENGTH + jnp.min(draws, axis=2)
    forced = jax.random.randint(forced_key, (STREAMS, 1), 0, N_ROWS)
    keep = jnp.where(jnp.arange(N_ROWS)[None, :] == forced, SPAN_LENGTH, keep)
    keys = jax.random.split(perm_key, STREAMS * N_ROWS)
    perms = jax.vmap(lambda single: jax.random.permutation(single, ROWS_DEV))(keys)
    perms = perms.reshape(STREAMS, N_ROWS, ROWS_DEV)
    mask = (perms < keep[:, :, None]).astype(jnp.int32)
    return mask.reshape(STREAMS, N_ROWS * ROWS_DEV)


def setup_inputs(seed: int = 0) -> dict:
    streams_of = jax.random.split(jax.random.key(seed), 3)
    return {
        "events": draw_events(jax.random.fold_in(streams_of[2], 71), 0),
        "keep_indicator": draw_keep_indicator(jax.random.fold_in(streams_of[2], 71), 0),
    }


def single_table_input(pair):
    values, persisting_flags = pair
    feature_width = values.shape[0]
    total_rows = values.shape[1]
    retained_rows = values * persisting_flags[None, :].astype(jnp.float32)
    order = jnp.argsort(1 - persisting_flags, stable=True).astype(jnp.int32)
    packed_entries = jnp.take(retained_rows, order, axis=1)
    extended = jnp.concatenate([jnp.zeros((feature_width, SPAN_LENGTH), jnp.float32), packed_entries], axis=1)
    blocks = extended.reshape(feature_width, (total_rows + SPAN_LENGTH) // SPAN_LENGTH, SPAN_LENGTH)
    partial_sums = jnp.cumsum(blocks, axis=2)
    whole = partial_sums[:, :, -1]
    trailing = partial_sums[:, 1:, :] + (whole[:, :-1, None] - partial_sums[:, :-1, :])
    trailing = trailing.reshape(feature_width, total_rows)
    remaining_position = jnp.cumsum(persisting_flags).astype(jnp.int32)
    gather_slot = jnp.maximum(remaining_position - 1, 0).astype(jnp.int32)
    selected_entries = jnp.take(trailing, gather_slot, axis=1)
    lagging_mean = jnp.where(remaining_position[None, :] >= 1, selected_entries, jnp.float32(0.0)) / SPAN_LENGTH
    local = jnp.cumsum(retained_rows.reshape(feature_width, N_ROWS, ROWS_DEV), axis=2)
    ends = local[:, :, -1]
    starts = jnp.cumsum(ends, axis=1) - ends
    running = (local + starts[:, :, None]).reshape(feature_width, total_rows)
    visited_tally = jnp.maximum(remaining_position.astype(jnp.float32), 1.0)
    deviation = lagging_mean - running / visited_tally[None, :]
    return lagging_mean, deviation


def reference(events, keep_indicator):
    lagging_mean, deviation = lax.map(single_table_input, (events, keep_indicator))
    return (lagging_mean, deviation)
```

```python
import functools

import jax
import jax.numpy as jnp
from jax import lax
from jax.experimental import pallas as pl
from jax.experimental.pallas import tpu as pltpu
from jax.sharding import PartitionSpec as P

SPAN = 4096
LANES = 128
GROUP = 16
GRANT = 16 * 2**20
MESH = pl.DeviceIdType.MESH
F32, BF16, I32 = jnp.float32, jnp.bfloat16, jnp.int32


def iota(shape, axis):
    return lax.broadcasted_iota(I32, shape, axis)


def lane_gather(values, index):
    return jnp.take_along_axis(values, index, axis=1, mode="promise_in_bounds")


def index_kernel(tiles, keep_ref, rank_ref, slot_ref, scalars_ref, flags):
    streams = keep_ref.shape[0]
    rows = streams * tiles
    for s in range(streams):
        for t in range(tiles):
            flags[s * tiles + t : s * tiles + t + 1, :] = keep_ref[s : s + 1, t * LANES : (t + 1) * LANES]
    kept = flags[...].astype(F32).astype(BF16)
    square = (LANES, LANES)
    upper = (iota(square, 0) <= iota(square, 1)).astype(F32).astype(BF16)
    ones = jnp.ones(square, BF16)
    within = jnp.dot(kept, upper, preferred_element_type=F32)
    counts = jnp.dot(kept, ones, preferred_element_type=F32).astype(BF16)
    grid = (rows, rows)
    same = (iota(grid, 0) // tiles) == (iota(grid, 1) // tiles)
    below = (same & (iota(grid, 1) < iota(grid, 0))).astype(F32).astype(BF16)
    above = (same & (iota(grid, 0) < iota(grid, 1))).astype(F32).astype(BF16)
    start = jnp.dot(below, counts, preferred_element_type=F32).astype(I32)
    within = within.astype(I32)
    rank_ref[...] = start + within
    lane = iota((rows, LANES), 1)
    wanted = ((lane - start - 1) & (LANES - 1)) + 1
    position = jnp.zeros((rows, LANES), I32)
    step = LANES // 2
    while step:
        seen = lane_gather(within, position + (step - 1))
        position = jnp.where(seen < wanted, position + step, position)
        step //= 2
    slot_ref[...] = position
    contract = (((1,), (1,)), ((), ()))
    first = (iota((8, LANES), 1) == 0).astype(F32).astype(BF16)
    count_row = lax.dot_general(jnp.ones((8, LANES), BF16), kept, contract, preferred_element_type=F32)
    first_row = lax.dot_general(first, kept, contract, preferred_element_type=F32)
    count_row = count_row.astype(BF16)
    start_row = jnp.dot(count_row, above, preferred_element_type=F32)
    total_row = jnp.dot(count_row, same.astype(F32).astype(BF16), preferred_element_type=F32)
    which = iota((8, rows), 0)
    row = jnp.where(which == 0, start_row, jnp.where(which == 1, total_row, start_row + first_row))
    scalars_ref[...] = row.astype(I32)


def head_kernel(count, tiles, scalars_ref, *refs):
    prefix_refs = refs[:-5]
    before_ref, mine, slots, send_sems, recv_sems = refs[-5:]
    streams = len(prefix_refs)
    cols = prefix_refs[0].shape[1]
    width = streams * cols
    me = lax.axis_index("rows")
    barrier = pltpu.get_barrier_semaphore()

    def greet(j, carry):
        @pl.when(j < me)
        def _():
            pl.semaphore_signal(barrier, inc=1, device_id=(j,), device_id_type=MESH)

        return carry

    lax.fori_loop(0, count, greet, 0)
    last = iota((cols, LANES), 1) == LANES - 1
    totals = [jnp.where(last, ref[tiles - 1], 0.0) for ref in prefix_refs]
    sums = lax.dot_general(
        jnp.ones((8, LANES), F32),
        jnp.concatenate(totals, axis=0),
        (((1,), (1,)), ((), ())),
        precision=lax.Precision.HIGHEST,
        preferred_element_type=F32,
    )
    row, column = iota((8, width), 0), iota((8, width), 1)
    counts = jnp.zeros((8, width), F32)
    for s in range(streams):
        counts = jnp.where(column // cols == s, scalars_ref[1, s * tiles].astype(F32), counts)
    mine[...] = jnp.where(row == 0, sums, counts)
    before_ref[...] = jnp.zeros((8, width), F32)

    @pl.when(me < count - 1)
    def _():
        pl.semaphore_wait(barrier, count - 1 - me)

    def copy(j, sender):
        return pltpu.make_async_remote_copy(
            src_ref=mine,
            dst_ref=slots.at[sender],
            send_sem=send_sems.at[j],
            recv_sem=recv_sems.at[sender],
            device_id=(j,),
            device_id_type=MESH,
        )

    def send(j, carry):
        @pl.when(j > me)
        def _():
            copy(j, me).start()

        return carry

    lax.fori_loop(0, count, send, 0)

    def receive(j, carry):
        @pl.when(j < me)
        def _():
            copy(j, j).wait_recv()
            before_ref[...] += slots[j]

        return carry

    def finish(j, carry):
        @pl.when(j > me)
        def _():
            copy(j, me).wait_send()

        return carry

    lax.fori_loop(0, count, receive, 0)
    lax.fori_loop(0, count, finish, 0)


def first_pack_kernel(s, tiles, group, scalars_ref, events_ref, keep_ref, slot_ref, *rest):
    prefix_ref, table_ref, send_ref = rest[-3:]
    cols = prefix_ref.shape[1]
    lane = iota((cols, LANES), 1)
    shape = (2 * LANES, 2 * LANES)
    weights = (((iota(shape, 0) & (LANES - 1)) <= iota(shape, 1)).astype(F32)).astype(BF16)
    total = jnp.zeros((cols, LANES), F32)
    current = jnp.zeros((cols, LANES), F32)
    for g in range(tiles // group):
        left, right = [], []
        for i in range(group):
            columns = slice((g * group + i) * LANES, (g * group + i + 1) * LANES)
            values = jnp.where(keep_ref[s : s + 1, columns] != 0, events_ref[s, :, columns], 0.0)
            high = values.astype(BF16)
            left.append(high)
            right.append((values - high.astype(F32)).astype(BF16))
        pair = jnp.concatenate([jnp.concatenate(left, axis=0), jnp.concatenate(right, axis=0)], axis=1)
        sums = jnp.dot(pair, weights, preferred_element_type=F32)
        for i in range(group):
            t = g * group + i
            piece = sums[i * cols : (i + 1) * cols]
            running = piece[:, :LANES] + total
            total = total + piece[:, LANES:]
            prefix_ref[t] = running
            order = jnp.broadcast_to(slot_ref[s * tiles + t : s * tiles + t + 1, :], (cols, LANES))
            packed = lane_gather(running, order)
            begin = scalars_ref[0, s * tiles + t] + 1
            block = begin // LANES
            merged = jnp.where(lane >= begin - block * LANES, packed, current)
            table_ref[block] = merged
            if t == tiles - 1:
                table_ref[block + 1] = packed
            else:
                following = (scalars_ref[0, s * tiles + t + 1] + 1) // LANES
                current = jnp.where(following > block, packed, merged)
    base = scalars_ref[1, s * tiles] - SPAN
    origin = base // LANES
    offset = base - origin * LANES
    turn = (lane + offset) & (LANES - 1)
    below = table_ref[origin]
    for m in range(SPAN // LANES):
        above = table_ref[origin + m + 1]
        send_ref[m] = lane_gather(jnp.where(lane >= offset, below, above), turn) - total
        below = above


def spread_kernel(s, tiles, group, scalars_ref, before_ref, rank_ref, prefix_ref, table_ref, tail_ref, *rest):
    mean_ref, deviation_ref, means, deviations, inverse, sems = rest[-6:]
    cols = prefix_ref.shape[1]
    back = SPAN // LANES
    width = before_ref.shape[1]
    mine = iota((cols, width), 1) == iota((cols, width), 0) + s * cols
    column = jnp.sum(jnp.where(mine, before_ref[0:1, :], 0.0), axis=1, keepdims=True)
    before = jnp.broadcast_to(column, (cols, LANES))
    first = iota((1, width), 1) == s * cols
    earlier = jnp.sum(jnp.where(first, before_ref[1:2, :], 0.0), axis=1, keepdims=True)
    ranks = rank_ref[s * tiles : (s + 1) * tiles, :]
    inverse[...] = 1.0 / jnp.maximum(earlier + ranks.astype(F32), 1.0)
    lane = iota((cols, LANES), 1)

    def fetch(block):
        old = tail_ref[jnp.minimum(block, back - 1)]
        new = table_ref[jnp.maximum(block - back, 0)]
        return jnp.where(block < back, old, new)

    copies = []
    for g in range(tiles // group):
        for i in range(group):
            t = g * group + i
            begin = scalars_ref[2, s * tiles + t]
            block = begin // LANES
            mixed = jnp.where(lane >= begin - block * LANES, fetch(block), fetch(block + 1))
            order = jnp.broadcast_to(rank_ref[s * tiles + t : s * tiles + t + 1, :] & (LANES - 1), (cols, LANES))
            running = prefix_ref[t]
            mean = (running - lane_gather(mixed, order)) * (1.0 / SPAN)
            columns = slice(t * LANES, (t + 1) * LANES)
            means[:, columns] = mean
            deviations[:, columns] = mean - (running + before) * inverse[t : t + 1, :]
        part = pl.ds(g * group * LANES, group * LANES)
        for k, (source, target) in enumerate(((means, mean_ref), (deviations, deviation_ref))):
            copy = pltpu.make_async_copy(source.at[:, part], target.at[s, :, part], sems.at[k, g])
            copy.start()
            copies.append(copy)
    for copy in copies:
        copy.wait()


def per_device(count, events, keep):
    streams, cols, rows = events.shape
    tiles = rows // LANES
    back = SPAN // LANES
    everything = streams * tiles
    width = streams * cols
    group = min(GROUP, tiles)
    smem = pl.BlockSpec(memory_space=pltpu.SMEM)
    vmem = pl.BlockSpec(memory_space=pltpu.VMEM)
    anywhere = pl.BlockSpec(memory_space=pl.ANY)
    cost = pl.CostEstimate(flops=10**9, bytes_accessed=8 * 2**20, transcendentals=0)
    params = pltpu.CompilerParams(vmem_limit_bytes=GRANT)

    rank, slot, scalars = pl.pallas_call(
        functools.partial(index_kernel, tiles),
        out_shape=(
            jax.ShapeDtypeStruct((everything, LANES), I32),
            jax.ShapeDtypeStruct((everything, LANES), I32),
            jax.ShapeDtypeStruct((8, everything), I32),
        ),
        scratch_shapes=[pltpu.VMEM((everything, LANES), I32)],
        cost_estimate=cost,
        compiler_params=params,
        name="index",
    )(keep)

    links = [(i, i + 1) for i in range(count - 1)]
    prefixes, tables, tails = [], [], []
    for s in range(streams):
        prefix, table, send = pl.pallas_call(
            functools.partial(first_pack_kernel, s, tiles, group),
            in_specs=[smem, vmem, vmem, vmem] + [anywhere] * (s > 0),
            out_specs=[vmem] * 3,
            out_shape=[
                jax.ShapeDtypeStruct((tiles, cols, LANES), F32),
                jax.ShapeDtypeStruct((tiles + 2, cols, LANES), F32),
                jax.ShapeDtypeStruct((back, cols, LANES), F32),
            ],
            cost_estimate=cost,
            compiler_params=params,
            name=f"pack{s}",
        )(scalars, events, keep, slot, *tables[-1:])
        prefixes.append(prefix)
        tables.append(table)
        tails.append(lax.ppermute(send, "rows", links))

    before = pl.pallas_call(
        functools.partial(head_kernel, count, tiles),
        in_specs=[smem] + [vmem] * streams,
        out_specs=vmem,
        out_shape=jax.ShapeDtypeStruct((8, width), F32),
        scratch_shapes=[
            pltpu.VMEM((8, width), F32),
            pltpu.VMEM((count, 8, width), F32),
            pltpu.SemaphoreType.DMA((count,)),
            pltpu.SemaphoreType.DMA((count,)),
        ],
        cost_estimate=cost,
        compiler_params=pltpu.CompilerParams(collective_id=0, has_side_effects=True, vmem_limit_bytes=GRANT),
        name="head",
    )(scalars, *prefixes)

    outs = ()
    for s in range(streams):
        outs = pl.pallas_call(
            functools.partial(spread_kernel, s, tiles, group),
            in_specs=[smem] + [vmem] * 5 + [anywhere] * len(outs),
            out_specs=[anywhere] * 2,
            out_shape=[jax.ShapeDtypeStruct(events.shape, F32)] * 2,
            scratch_shapes=[
                pltpu.VMEM((cols, rows), F32),
                pltpu.VMEM((cols, rows), F32),
                pltpu.VMEM((tiles, LANES), F32),
                pltpu.SemaphoreType.DMA((2, tiles // group)),
            ],
            input_output_aliases={6: 0, 7: 1} if outs else {},
            cost_estimate=cost,
            compiler_params=params,
            name=f"spread{s}",
        )(scalars, before, rank, prefixes[s], tables[s], tails[s], *outs)
    return tuple(outs)


def solution(mesh):
    return jax.shard_map(
        functools.partial(per_device, mesh.shape["rows"]),
        mesh=mesh,
        in_specs=(P(None, None, "rows"), P(None, "rows")),
        out_specs=(P(None, None, "rows"), P(None, None, "rows")),
        check_vma=False,
    )
```
